32 devices in a mesh: ka: 4 (over y, x), ga: 8 (over z, core).
Axes of the slice: x: 2, y: 2, z: 4, core: 2. Of those that a mesh axis runs over, the one named last changes fastest.
Arguments:
- orbitals: bfloat16 [8, 8, 2, 32, 1024], P('ka', None, None, 'ga'), may hold values from -6 to 6
- band_counts: int32 [8], replicated, may hold values from 1 to 8, as said below
- pair_slot: int32 [8, 8], replicated, may hold values from 0 to 7
- kernel: float32 [8, 32, 1024], P(None, None, 'ga'), may hold values from 0.2 to 8
Outputs:
- exchange_vectors: float32 [8, 8, 2, 32, 1024], P('ka', None, None, 'ga')
- exchange_matrix: float32 [8, 2, 8, 8], P('ka')
- exchange_energy: float32 [], replicated
The draws below stay inside these ranges and needn't reach their ends.
Inputs may be any that keep to these rules, and one draw needn't show every extreme that they name: The first band_counts[k] band slots of k-point k are the occupied ones; some k-point has all 8 slots occupied.
All inputs are finite; a program needn't handle non-finite values.
Results may differ from the reference program's by a relative error of at most 0.0003.
Values may be sent and summed in bfloat16 or wider, within the bound.
A program may use at most 128 MiB of HBM per device.

```python
import math
import jax
import jax.numpy as jnp
from jax import lax

G = 32
K_DEV = 2
BANDS = 8
STEPS = 2
KPOINTS = 8
N_KA = 4


def draw_band_counts(key, part):
    first_key, second_key, third_key = jax.random.split(key, 3)
    partial_fill = jax.random.randint(first_key, (KPOINTS,), 1, BANDS // 2 + 1)
    full_mark = jax.random.randint(second_key, (KPOINTS,), 0, 4) == 0
    counts = jnp.where(full_mark, BANDS, partial_fill)
    chosen = jax.random.randint(third_key, (), 0, KPOINTS)
    positions = jnp.arange(KPOINTS)
    counts = jnp.where(positions == chosen, BANDS, counts)
    return counts.astype(jnp.int32)


def with_ends(array, own_key, low, top_value):
    longest = array.shape.index(max(array.shape))
    spots = []
    for shift in (0, 1):
        where = [jax.random.randint(jax.random.fold_in(own_key, axis), (), 0, length) for axis, length in enumerate(array.shape)]
        where[longest] = (where[longest] + shift) % array.shape[longest]
        spots.append(tuple(where))
    return array.at[spots[0]].set(low).at[spots[1]].set(top_value)


def level_of(stream_key, extent, cuts, least, high):
    def one(axis_at, parts):
        steps = jax.random.uniform(jax.random.fold_in(jax.random.fold_in(stream_key, 6), axis_at), (parts,), jnp.float32, least / len(cuts), high / len(cuts))
        return jnp.repeat(jnp.exp(steps), extent[axis_at] // parts).reshape((-1,) + (1,) * (len(extent) - axis_at - 1))

    factor_of = one(*cuts[0])
    for cut in cuts[1:]:
        factor_of = factor_of * one(*cut)
    return factor_of


def gaussian(own_key, dims, scale, bound, cuts=(), kind=jnp.bfloat16):
    values = jax.random.normal(own_key, dims, jnp.float32) * scale
    if len(cuts) > 0:
        values = level_of(own_key, dims, cuts, -0.22, 0.18) * values
    return jnp.clip(values, min=-bound, max=bound).astype(kind)


def setup_inputs(seed: int = 0) -> dict:
    keys = jax.random.split(jax.random.key(seed), 5)
    orbitals = gaussian(keys[0], (KPOINTS, BANDS, 2, G, G * G), 1.0, 6.0, ((0, 4), (3, 8)))
    band_counts = draw_band_counts(jax.random.fold_in(keys[4], 71), 0)
    pair_slot = with_ends(jax.random.randint(keys[2], (KPOINTS, KPOINTS), 0, KPOINTS), jax.random.fold_in(keys[2], 1), 0, KPOINTS - 1).astype(jnp.int32)
    kernel = jnp.clip(jnp.exp(math.log(8.0) - 3.6888794 * jax.random.uniform(keys[3], (KPOINTS, G, G * G), jnp.float32) ** level_of(keys[3], (KPOINTS, G, G * G), ((2, 8),), -0.2, 0.2)), 0.2, 8.0)
    return dict(orbitals=orbitals, band_counts=band_counts, pair_slot=pair_slot, kernel=kernel)


highest = lax.Precision.HIGHEST


def contract(first_field, second_field):
    return jnp.einsum("kar,kbr->kab", first_field, second_field, precision=highest)


def reference(orbitals, band_counts, pair_slot, kernel):
    kpoints = orbitals.shape[0]
    band_count = orbitals.shape[1]
    points = orbitals.shape[3]
    volume = points * points * points
    occupied = (jnp.arange(band_count, dtype=jnp.int32)[None, :] < band_counts[:, None]).astype(jnp.float32)
    real_part = orbitals[:, :, 0].astype(jnp.float32)
    imag_part = orbitals[:, :, 1].astype(jnp.float32)
    grid_shape = (kpoints, band_count, points, points, points)
    orbital_field = lax.complex(real_part, imag_part).reshape(grid_shape)
    spectra_kernel = kernel.reshape(kpoints, points, points, points)

    def one_kpoint(kpoint):
        own_group = kpoint // K_DEV
        own_field = orbital_field[kpoint]
        total_real = jnp.zeros((band_count, points, points, points), jnp.float32)
        total_imag = jnp.zeros((band_count, points, points, points), jnp.float32)
        for rotation in range(STEPS):
            anchor = (own_group - rotation) % N_KA
            window = (anchor * K_DEV + jnp.arange(K_DEV, dtype=jnp.int32)).astype(jnp.int32)
            partner = orbital_field[window] * occupied[window][:, :, None, None, None]
            density = jnp.conj(partner)[None] * own_field[:, None, None]
            spectra = jnp.fft.fftn(density, axes=(3, 4, 5))
            chosen = spectra_kernel[pair_slot[kpoint, window]]
            potential = jnp.fft.ifftn(spectra * chosen[None, :, None], axes=(3, 4, 5))
            product_field = jnp.sum(partner[None] * potential, axis=(1, 2))
            total_real = total_real + jnp.real(product_field)
            total_imag = total_imag + jnp.imag(product_field)
        prefactor = -1.0 / kpoints
        stacked = jnp.stack((total_real, total_imag), axis=1)
        return stacked.reshape(band_count, 2, points, points * points) * prefactor

    exchange_vectors = lax.map(one_kpoint, jnp.arange(kpoints, dtype=jnp.int32))
    flat_orbitals = orbitals.astype(jnp.float32).reshape(kpoints, band_count, 2, volume)
    flat_vectors = exchange_vectors.reshape(kpoints, band_count, 2, volume)
    matrix_real = (contract(flat_orbitals[:, :, 0], flat_vectors[:, :, 0]) + contract(flat_orbitals[:, :, 1], flat_vectors[:, :, 1])) / volume
    matrix_imag = (contract(flat_orbitals[:, :, 0], flat_vectors[:, :, 1]) - contract(flat_orbitals[:, :, 1], flat_vectors[:, :, 0])) / volume
    exchange_matrix = jnp.stack((matrix_real, matrix_imag), axis=1)
    exchange_energy = jnp.sum(occupied * jnp.diagonal(matrix_real, axis1=1, axis2=2)) / (2.0 * kpoints)
    return exchange_vectors, exchange_matrix, exchange_energy
```

```python
import jax
import jax.numpy as jnp
import numpy as np
from jax import lax
from jax.experimental import pallas as pl
from jax.experimental.pallas import tpu as pltpu
from jax.sharding import PartitionSpec as P

STEPS = 2
LANES = 128


def split_np(matrix):
    high = matrix.astype(np.float32).astype(jnp.bfloat16)
    low = (matrix - high.astype(np.float64)).astype(np.float32).astype(jnp.bfloat16)
    return high, low


def real_form(matrix):
    return np.block([[matrix.real, -matrix.imag], [matrix.imag, matrix.real]])


def build_tables(points, members):
    wide = LANES // points
    quads = points // (2 * wide)
    planes = points // members
    dft = np.exp(-2j * np.pi * np.outer(np.arange(points), np.arange(points)) / points)
    x_of = np.arange(points).reshape(members, 1, planes)
    y1_of = np.arange(quads).reshape(1, quads, 1)
    x_of, y1_of = (np.broadcast_to(v, (members, quads, planes)).reshape(-1) for v in (x_of, y1_of))
    gx = np.tile(np.arange(points), quads)
    q = np.repeat(np.arange(quads), points)
    left, left_back = [], []
    for p in range(2):
        phase = np.outer(gx, x_of) / points + np.outer(p + 2 * q, y1_of) * wide / points
        forward = np.exp(-2j * np.pi * phase)
        high, low = split_np(real_form(forward))
        left.append(np.concatenate([high, low, high], axis=1))
        high, low = split_np(real_form(np.conj(forward).T))
        left_back.append(np.concatenate([high, low, high], axis=1))
    small = np.exp(-2j * np.pi * np.outer(np.arange(wide), np.arange(wide)) / wide)
    lane = np.kron(small, dft)
    right = []
    for matrix in (lane, np.conj(lane)):
        high, low = split_np(real_form(matrix).T)
        right.append(np.concatenate([high, low, high], axis=0))
    low_freq = (np.arange(2)[:, None] + 2 * np.arange(quads)[None, :]).reshape(-1)
    y0 = np.repeat(np.arange(wide), points)
    twiddle = np.exp(-2j * np.pi * np.outer(low_freq, y0) / points)
    twiddle = np.stack([twiddle.real, twiddle.imag]).astype(np.float32)
    return np.stack(left), np.stack(left_back), right[0], right[1], twiddle


def split(values):
    high = values.astype(jnp.bfloat16)
    low = (values - high.astype(jnp.float32)).astype(jnp.bfloat16)
    return high, low


def pair_kernel(rows, bands, windows, points, info, block, kernel, left, left_back, right, right_back,
                twiddle, out, projections, own, other, total):
    members = block.shape[0]
    piece = block.shape[3] // 2
    tall = members * piece
    quads = tall // points

    def load(orbital, part, h):
        value = block[:, orbital, part, h * piece:(h + 1) * piece, :]
        return value.astype(jnp.float32).reshape(tall, LANES)

    first_row = info[2 * windows]
    first_band = info[2 * windows + 1]
    for r in range(rows):
        for part in range(2):
            for h in range(2):
                own[r, part, h] = load(first_row + r, part, h)
    total[...] = jnp.zeros_like(total)

    def rotate(real_part, imag_part, p, sign):
        cos = twiddle[0, p * quads:(p + 1) * quads, :].reshape(quads, 1, LANES)
        sin = twiddle[1, p * quads:(p + 1) * quads, :].reshape(quads, 1, LANES) * sign
        real_part = real_part.reshape(quads, points, LANES)
        imag_part = imag_part.reshape(quads, points, LANES)
        new_real = real_part * cos - imag_part * sin
        new_imag = imag_part * cos + real_part * sin
        return new_real.reshape(tall, LANES), new_imag.reshape(tall, LANES)

    def dot(a, b):
        return jnp.dot(a, b, preferred_element_type=jnp.float32)

    def from_left(matrix, values):
        high, low = split(values)
        return dot(matrix, jnp.concatenate([high, high, low], axis=0))

    def from_right(values, matrix):
        high, low = split(values)
        return dot(jnp.concatenate([high, high, low], axis=1), matrix)

    def window_body(w, carry):
        slot = info[windows + w]

        def band_body(b, carry):
            orbital = w * bands + b
            for part in range(2):
                for h in range(2):
                    other[part, h] = load(orbital, part, h)
            inputs = ([], [])
            for r in range(rows):
                fields = []
                for h in range(2):
                    real_part = own[r, 0, h] * other[0, h] + own[r, 1, h] * other[1, h]
                    imag_part = own[r, 1, h] * other[0, h] - own[r, 0, h] * other[1, h]
                    fields.append(jnp.concatenate([real_part, imag_part], axis=0))
                inputs[0].append(fields[0] + fields[1])
                inputs[1].append(fields[0] - fields[1])
            turned = []
            for p in range(2):
                spectrum = from_left(left[p], jnp.concatenate(inputs[p], axis=1))
                for r in range(rows):
                    cut = spectrum[:, r * LANES:(r + 1) * LANES]
                    turned.append(jnp.concatenate(rotate(cut[:tall], cut[tall:], p, 1.0), axis=1))
            back = ([], [])
            for p in range(2):
                chosen = kernel[slot, p * tall:(p + 1) * tall, :]
                chosen = jnp.concatenate([chosen, chosen], axis=1)
                for r in range(rows):
                    full = from_right(turned[p * rows + r], right[...]) * chosen
                    full = from_right(full, right_back[...])
                    pair = rotate(full[:, :LANES], full[:, LANES:], p, -1.0)
                    back[p].append(jnp.concatenate(pair, axis=0))
            halves = [from_left(left_back[p], jnp.concatenate(back[p], axis=1)) for p in range(2)]
            for h in range(2):
                potential = halves[0] + halves[1] if h == 0 else halves[0] - halves[1]
                for r in range(rows):
                    real_part = potential[:tall, r * LANES:(r + 1) * LANES]
                    imag_part = potential[tall:, r * LANES:(r + 1) * LANES]
                    total[r, 0, h] += other[0, h] * real_part - other[1, h] * imag_part
                    total[r, 1, h] += other[0, h] * imag_part + other[1, h] * real_part
            return carry

        return lax.fori_loop(0, info[w], band_body, carry)

    lax.fori_loop(0, windows, window_body, 0)
    for r in range(rows):
        for part in range(2):
            for h in range(2):
                out[:, r, part, h * piece:(h + 1) * piece, :] = total[r, part, h].reshape(members, piece, LANES)

    def project(a, carry):
        for part in range(2):
            for h in range(2):
                other[part, h] = load(first_band + a, part, h)
        for r in range(rows):
            real_sum = jnp.zeros((tall, LANES), jnp.float32)
            imag_sum = jnp.zeros((tall, LANES), jnp.float32)
            for h in range(2):
                real_sum += other[0, h] * total[r, 0, h] + other[1, h] * total[r, 1, h]
                imag_sum += other[0, h] * total[r, 1, h] - other[1, h] * total[r, 0, h]
            projections[r, a] = jnp.concatenate(
                [jnp.sum(real_sum, axis=0, keepdims=True), jnp.sum(imag_sum, axis=0, keepdims=True)], axis=0)
        return carry

    lax.fori_loop(0, bands, project, 0)


def on_device(orbitals, band_counts, pair_slot, kernel):
    local, bands, _, planes, columns = orbitals.shape
    slots, points = kernel.shape[0], kernel.shape[1]
    members = lax.axis_size("ga")
    groups = lax.axis_size("ka")
    kpoints = local * groups
    group, member = lax.axis_index("ka"), lax.axis_index("ga")
    volume = float(points ** 3)
    wide = LANES // points
    quads = points // (2 * wide)
    tiles = columns // LANES
    rows = max(1, local * bands // members)
    share = max(1, members // (local * bands))
    windows = STEPS * local
    tables = build_tables(points, members)

    pieces = orbitals.reshape(local * bands, 2, planes, tiles, LANES).transpose(0, 1, 3, 2, 4)
    pieces = pieces.reshape(local * bands, 2, tiles * planes, LANES)
    blocks = [pieces]
    pairs = [(source, (source + 1) % groups) for source in range(groups)]
    for _ in range(STEPS - 1):
        blocks.append(lax.ppermute(blocks[-1], "ka", pairs))
    gathered = lax.all_gather(jnp.concatenate(blocks, axis=0), "ga", axis=0)

    whole = lax.all_gather(kernel, "ga", axis=2, tiled=True) * (-1.0 / (kpoints * volume))
    whole = whole.reshape(slots, points, wide, quads, 2, points).transpose(0, 4, 3, 1, 2, 5)
    whole = whole.reshape(slots, 2 * quads * points, LANES)

    first_row = member // share * rows
    own_kpoint = first_row // bands
    anchors = (group - jnp.arange(STEPS, dtype=jnp.int32)) % groups
    window = (anchors[:, None] * local + jnp.arange(local, dtype=jnp.int32)[None, :]).reshape(-1)
    slot_row = lax.dynamic_index_in_dim(pair_slot, group * local + own_kpoint, 0, keepdims=False)
    mine = jnp.arange(windows, dtype=jnp.int32) % share == member % share
    info = jnp.concatenate([jnp.where(mine, band_counts[window], 0), slot_row[window],
                            jnp.stack([first_row, own_kpoint * bands]).astype(jnp.int32)])

    tall = quads * points
    field = (rows, 2, 2, tall, LANES)
    smem = pl.BlockSpec(memory_space=pltpu.SMEM)
    vmem = pl.BlockSpec(memory_space=pltpu.VMEM)

    def body(*refs):
        pair_kernel(rows, bands, windows, points, *refs)

    spread, projections = pl.pallas_call(
        body,
        out_shape=(jax.ShapeDtypeStruct((members, rows, 2, tiles * planes, LANES), jnp.float32),
                   jax.ShapeDtypeStruct((rows, bands, 2, LANES), jnp.float32)),
        in_specs=[smem] + [vmem] * 7,
        out_specs=(vmem, vmem),
        scratch_shapes=[pltpu.VMEM(field, jnp.float32), pltpu.VMEM(field[1:], jnp.float32),
                        pltpu.VMEM(field, jnp.float32)],
        compiler_params=pltpu.CompilerParams(vmem_limit_bytes=48 * 2 ** 20),
        name="pairs",
    )(info, gathered, whole, *[jnp.asarray(table) for table in tables])

    vectors = lax.all_to_all(spread, "ga", split_axis=0, concat_axis=0, tiled=True)
    if share > 1:
        vectors = jnp.sum(vectors.reshape(local * bands, share, *vectors.shape[1:]), axis=1)
    vectors = vectors.reshape(local, bands, 2, tiles, planes, LANES).transpose(0, 1, 2, 4, 3, 5)
    vectors = vectors.reshape(local, bands, 2, planes, columns)
    sums = jnp.sum(projections, axis=-1) / volume
    sums = lax.all_gather(sums, ("ka", "ga"), axis=0)
    sums = jnp.sum(sums.reshape(kpoints, bands, share, bands, 2), axis=2)
    everything = sums.transpose(0, 3, 2, 1)
    matrix = lax.dynamic_slice_in_dim(everything, group * local, local, 0)
    occupied = (jnp.arange(bands)[None, :] < band_counts[:, None]).astype(jnp.float32)
    energy = jnp.sum(occupied * jnp.diagonal(everything[:, 0], axis1=1, axis2=2)) / (2.0 * kpoints)
    return (vectors, matrix, energy)


def solution(mesh):
    in_specs = (P("ka", None, None, "ga", None), P(), P(), P(None, None, "ga"))
    out_specs = (P("ka", None, None, "ga", None), P("ka", None, None, None), P())
    return jax.shard_map(
        on_device, mesh=mesh, in_specs=in_specs, out_specs=out_specs, check_vma=False
    )
```

```python
import jax
import jax.numpy as jnp
import numpy as np
from jax import lax
from jax.experimental import pallas as pl
from jax.experimental.pallas import tpu as pltpu
from jax.sharding import PartitionSpec as P

STEPS = 2
LANES = 128


def split_np(matrix):
    high = matrix.astype(np.float32).astype(jnp.bfloat16)
    low = (matrix - high.astype(np.float64)).astype(np.float32).astype(jnp.bfloat16)
    return high, low


def real_form(matrix):
    return np.block([[matrix.real, -matrix.imag], [matrix.imag, matrix.real]])


def build_tables(points, members):
    wide = LANES // points
    quads = points // (2 * wide)
    planes = points // members
    dft = np.exp(-2j * np.pi * np.outer(np.arange(points), np.arange(points)) / points)
    x_of = np.arange(points).reshape(members, 1, planes)
    y1_of = np.arange(quads).reshape(1, quads, 1)
    x_of, y1_of = (np.broadcast_to(v, (members, quads, planes)).reshape(-1) for v in (x_of, y1_of))
    gx = np.tile(np.arange(points), quads)
    q = np.repeat(np.arange(quads), points)
    left, left_back = [], []
    for p in range(2):
        phase = np.outer(gx, x_of) / points + np.outer(p + 2 * q, y1_of) * wide / points
        forward = np.exp(-2j * np.pi * phase)
        high, low = split_np(real_form(forward))
        left.append(np.concatenate([high, low, high], axis=1))
        high, low = split_np(real_form(np.conj(forward).T))
        left_back.append(np.concatenate([high, low, high], axis=1))
    small = np.exp(-2j * np.pi * np.outer(np.arange(wide), np.arange(wide)) / wide)
    lane = np.kron(small, dft)
    right = []
    for matrix in (lane, np.conj(lane)):
        high, low = split_np(real_form(matrix).T)
        right.append(np.concatenate([high, low, high], axis=0))
    low_freq = (np.arange(2)[:, None] + 2 * np.arange(quads)[None, :]).reshape(-1)
    y0 = np.repeat(np.arange(wide), points)
    twiddle = np.exp(-2j * np.pi * np.outer(low_freq, y0) / points)
    twiddle = np.stack([twiddle.real, twiddle.imag]).astype(np.float32)
    return np.stack(left), np.stack(left_back), right[0], right[1], twiddle


def split(values):
    high = values.astype(jnp.bfloat16)
    low = (values - high.astype(jnp.float32)).astype(jnp.bfloat16)
    return high, low


def pair_kernel(rows, bands, windows, points, first, last, info, *refs):
    mine, refs = refs[0], refs[1:]
    block, refs = (mine, refs) if first else (refs[0], refs[1:])
    before, refs = (None, refs) if first else (refs[0], refs[1:])
    kernel, left, left_back, right, right_back, twiddle, out = refs[:7]
    projections, refs = (refs[7], refs[8:]) if last else (None, refs[7:])
    own, other = refs[:2]
    total = refs[2] if last else out
    members = block.shape[0]
    piece = block.shape[3] // 2
    tall = members * piece
    quads = tall // points

    def load(orbital, part, h, source=block):
        value = source[:, orbital, part, h * piece:(h + 1) * piece, :]
        return value.astype(jnp.float32).reshape(tall, LANES)

    first_row = info[2 * windows]
    first_band = info[2 * windows + 1]
    for r in range(rows):
        for part in range(2):
            for h in range(2):
                own[r, part, h] = load(first_row + r, part, h, mine)
    total[...] = jnp.zeros_like(total) if first else before[...]

    def rotate(real_part, imag_part, p, sign):
        cos = twiddle[0, p * quads:(p + 1) * quads, :].reshape(quads, 1, LANES)
        sin = twiddle[1, p * quads:(p + 1) * quads, :].reshape(quads, 1, LANES) * sign
        real_part = real_part.reshape(quads, points, LANES)
        imag_part = imag_part.reshape(quads, points, LANES)
        new_real = real_part * cos - imag_part * sin
        new_imag = imag_part * cos + real_part * sin
        return new_real.reshape(tall, LANES), new_imag.reshape(tall, LANES)

    def dot(a, b):
        return jnp.dot(a, b, preferred_element_type=jnp.float32)

    def from_left(matrix, values):
        high, low = split(values)
        return dot(matrix, jnp.concatenate([high, high, low], axis=0))

    def from_right(values, matrix):
        high, low = split(values)
        return dot(jnp.concatenate([high, high, low], axis=1), matrix)

    def window_body(w, carry):
        slot = info[windows + w]

        def band_body(b, carry):
            orbital = w * bands + b
            for part in range(2):
                for h in range(2):
                    other[part, h] = load(orbital, part, h)
            inputs = ([], [])
            for r in range(rows):
                fields = []
                for h in range(2):
                    real_part = own[r, 0, h] * other[0, h] + own[r, 1, h] * other[1, h]
                    imag_part = own[r, 1, h] * other[0, h] - own[r, 0, h] * other[1, h]
                    fields.append(jnp.concatenate([real_part, imag_part], axis=0))
                inputs[0].append(fields[0] + fields[1])
                inputs[1].append(fields[0] - fields[1])
            turned = []
            for p in range(2):
                spectrum = from_left(left[p], jnp.concatenate(inputs[p], axis=1))
                for r in range(rows):
                    cut = spectrum[:, r * LANES:(r + 1) * LANES]
                    turned.append(jnp.concatenate(rotate(cut[:tall], cut[tall:], p, 1.0), axis=1))
            back = ([], [])
            for p in range(2):
                chosen = kernel[slot, p * tall:(p + 1) * tall, :]
                chosen = jnp.concatenate([chosen, chosen], axis=1)
                for r in range(rows):
                    full = from_right(turned[p * rows + r], right[...]) * chosen
                    full = from_right(full, right_back[...])
                    pair = rotate(full[:, :LANES], full[:, LANES:], p, -1.0)
                    back[p].append(jnp.concatenate(pair, axis=0))
            halves = [from_left(left_back[p], jnp.concatenate(back[p], axis=1)) for p in range(2)]
            for h in range(2):
                potential = halves[0] + halves[1] if h == 0 else halves[0] - halves[1]
                for r in range(rows):
                    real_part = potential[:tall, r * LANES:(r + 1) * LANES]
                    imag_part = potential[tall:, r * LANES:(r + 1) * LANES]
                    total[r, 0, h] += other[0, h] * real_part - other[1, h] * imag_part
                    total[r, 1, h] += other[0, h] * imag_part + other[1, h] * real_part
            return carry

        return lax.fori_loop(0, info[w], band_body, carry)

    lax.fori_loop(0, windows, window_body, 0)
    if not last:
        return
    for r in range(rows):
        for part in range(2):
            for h in range(2):
                out[:, r, part, h * piece:(h + 1) * piece, :] = total[r, part, h].reshape(members, piece, LANES)

    def project(a, carry):
        for part in range(2):
            for h in range(2):
                other[part, h] = load(first_band + a, part, h, mine)
        for r in range(rows):
            real_sum = jnp.zeros((tall, LANES), jnp.float32)
            imag_sum = jnp.zeros((tall, LANES), jnp.float32)
            for h in range(2):
                real_sum += other[0, h] * total[r, 0, h] + other[1, h] * total[r, 1, h]
                imag_sum += other[0, h] * total[r, 1, h] - other[1, h] * total[r, 0, h]
            projections[r, a] = jnp.concatenate(
                [jnp.sum(real_sum, axis=0, keepdims=True), jnp.sum(imag_sum, axis=0, keepdims=True)], axis=0)
        return carry

    lax.fori_loop(0, bands, project, 0)


def on_device(orbitals, band_counts, pair_slot, kernel):
    local, bands, _, planes, columns = orbitals.shape
    slots, points = kernel.shape[0], kernel.shape[1]
    members = lax.axis_size("ga")
    groups = lax.axis_size("ka")
    kpoints = local * groups
    group, member = lax.axis_index("ka"), lax.axis_index("ga")
    volume = float(points ** 3)
    wide = LANES // points
    quads = points // (2 * wide)
    tiles = columns // LANES
    rows = max(1, local * bands // members)
    share = max(1, members // (local * bands))
    tables = build_tables(points, members)

    pieces = orbitals.reshape(local * bands, 2, planes, tiles, LANES).transpose(0, 1, 3, 2, 4)
    pieces = pieces.reshape(local * bands, 2, tiles * planes, LANES)
    pairs = [(source, (source + 1) % groups) for source in range(groups)]
    blocks = [lax.all_gather(pieces, "ga", axis=0)]
    for _ in range(STEPS - 1):
        pieces = lax.ppermute(pieces, "ka", pairs)
        blocks.append(lax.all_gather(pieces, "ga", axis=0))

    whole = lax.all_gather(kernel, "ga", axis=2, tiled=True) * (-1.0 / (kpoints * volume))
    whole = whole.reshape(slots, points, wide, quads, 2, points).transpose(0, 4, 3, 1, 2, 5)
    whole = whole.reshape(slots, 2 * quads * points, LANES)

    first_row = member // share * rows
    own_kpoint = first_row // bands
    slot_row = lax.dynamic_index_in_dim(pair_slot, group * local + own_kpoint, 0, keepdims=False)
    mine = jnp.arange(local, dtype=jnp.int32) % share == member % share
    places = jnp.stack([first_row, own_kpoint * bands]).astype(jnp.int32)

    tall = quads * points
    field = (rows, 2, 2, tall, LANES)
    smem = pl.BlockSpec(memory_space=pltpu.SMEM)
    vmem = pl.BlockSpec(memory_space=pltpu.VMEM)

    tables = [jnp.asarray(table) for table in tables]
    state = []
    for step in range(STEPS):
        first, last = step == 0, step == STEPS - 1
        anchor = (group - step) % groups * local
        counts = lax.dynamic_slice_in_dim(band_counts, anchor, local)
        chosen = lax.dynamic_slice_in_dim(slot_row, anchor, local)
        info = jnp.concatenate([jnp.where(mine, counts, 0), chosen, places])
        operands = blocks[:1] + ([] if first else [blocks[step]] + state) + [whole] + tables
        results = [jax.ShapeDtypeStruct(field, jnp.float32)]
        scratch = [pltpu.VMEM(field, jnp.float32), pltpu.VMEM(field[1:], jnp.float32)]
        if last:
            results = [jax.ShapeDtypeStruct((members, rows, 2, tiles * planes, LANES), jnp.float32),
                       jax.ShapeDtypeStruct((rows, bands, 2, LANES), jnp.float32)]
            scratch.append(pltpu.VMEM(field, jnp.float32))

        def body(*refs, first=first, last=last):
            pair_kernel(rows, bands, local, points, first, last, *refs)

        state = list(pl.pallas_call(
            body,
            out_shape=results,
            in_specs=[smem] + [vmem] * len(operands),
            out_specs=[vmem] * len(results),
            scratch_shapes=scratch,
            compiler_params=pltpu.CompilerParams(vmem_limit_bytes=32 * 2 ** 20),
            cost_estimate=pl.CostEstimate(flops=20 * 10 ** 9, bytes_accessed=8 * 2 ** 20, transcendentals=0),
            name=f"pairs_{step}",
        )(info, *operands))
    spread, projections = state

    vectors = lax.all_to_all(spread, "ga", split_axis=0, concat_axis=0, tiled=True)
    if share > 1:
        vectors = jnp.sum(vectors.reshape(local * bands, share, *vectors.shape[1:]), axis=1)
    vectors = vectors.reshape(local, bands, 2, tiles, planes, LANES).transpose(0, 1, 2, 4, 3, 5)
    vectors = vectors.reshape(local, bands, 2, planes, columns)
    sums = jnp.sum(projections, axis=-1) / volume
    everything = jnp.zeros((kpoints, 2, bands, bands), jnp.float32)
    everything = lax.dynamic_update_slice(
        everything, sums.transpose(2, 1, 0)[None], (group * local + own_kpoint, 0, 0, first_row % bands))
    everything = lax.psum(everything, ("ka", "ga"))
    matrix = lax.dynamic_slice_in_dim(everything, group * local, local, 0)
    occupied = (jnp.arange(bands)[None, :] < band_counts[:, None]).astype(jnp.float32)
    energy = jnp.sum(occupied * jnp.diagonal(everything[:, 0], axis1=1, axis2=2)) / (2.0 * kpoints)
    return (vectors, matrix, energy)


def solution(mesh):
    in_specs = (P("ka", None, None, "ga", None), P(), P(), P(None, None, "ga"))
    out_specs = (P("ka", None, None, "ga", None), P("ka", None, None, None), P())
    return jax.shard_map(
        on_device, mesh=mesh, in_specs=in_specs, out_specs=out_specs, check_vma=False
    )
```

```python
import jax
import jax.numpy as jnp
import numpy as np
from jax import lax
from jax.experimental import pallas as pl
from jax.experimental.pallas import tpu as pltpu
from jax.sharding import PartitionSpec as P

STEPS = 2
LANES = 128


def split_np(matrix):
    high = matrix.astype(np.float32).astype(jnp.bfloat16)
    low = (matrix - high.astype(np.float64)).astype(np.float32).astype(jnp.bfloat16)
    return high, low


def real_form(matrix):
    return np.block([[matrix.real, -matrix.imag], [matrix.imag, matrix.real]])


def build_tables(points, members):
    wide = LANES // points
    quads = points // (2 * wide)
    planes = points // members
    dft = np.exp(-2j * np.pi * np.outer(np.arange(points), np.arange(points)) / points)
    x_of = np.arange(points).reshape(members, 1, planes)
    y1_of = np.arange(quads).reshape(1, quads, 1)
    x_of, y1_of = (np.broadcast_to(v, (members, quads, planes)).reshape(-1) for v in (x_of, y1_of))
    gx = np.tile(np.arange(points), quads)
    q = np.repeat(np.arange(quads), points)
    left, left_back = [], []
    for p in range(2):
        phase = np.outer(gx, x_of) / points + np.outer(p + 2 * q, y1_of) * wide / points
        forward = np.exp(-2j * np.pi * phase)
        high, low = split_np(real_form(forward))
        left.append(np.concatenate([high, low, high], axis=1))
        high, low = split_np(real_form(np.conj(forward).T))
        left_back.append(np.concatenate([high, low, high], axis=1))
    small = np.exp(-2j * np.pi * np.outer(np.arange(wide), np.arange(wide)) / wide)
    lane = np.kron(small, dft)
    right = []
    for matrix in (lane, np.conj(lane)):
        high, low = split_np(real_form(matrix).T)
        right.append(np.concatenate([high, low, high], axis=0))
    low_freq = (np.arange(2)[:, None] + 2 * np.arange(quads)[None, :]).reshape(-1)
    y0 = np.repeat(np.arange(wide), points)
    twiddle = np.exp(-2j * np.pi * np.outer(low_freq, y0) / points)
    twiddle = np.stack([twiddle.real, twiddle.imag]).astype(np.float32)
    return np.stack(left), np.stack(left_back), right[0], right[1], twiddle


def split(values):
    high = values.astype(jnp.bfloat16)
    low = (values - high.astype(jnp.float32)).astype(jnp.bfloat16)
    return high, low


def pair_kernel(rows, bands, windows, points, info, block, kernel, left, left_back, right, right_back,
                twiddle, out, projections, own, other, total):
    members = block.shape[0]
    piece = block.shape[3] // 2
    tall = members * piece
    quads = tall // points

    def load(orbital, part, h):
        value = block[:, orbital, part, h * piece:(h + 1) * piece, :]
        return value.astype(jnp.float32).reshape(tall, LANES)

    first_row = info[2 * windows]
    first_band = info[2 * windows + 1]
    for r in range(rows):
        for part in range(2):
            for h in range(2):
                own[r, part, h] = load(first_row + r, part, h)
    total[...] = jnp.zeros_like(total)

    def rotate(real_part, imag_part, p, sign):
        cos = twiddle[0, p * quads:(p + 1) * quads, :].reshape(quads, 1, LANES)
        sin = twiddle[1, p * quads:(p + 1) * quads, :].reshape(quads, 1, LANES) * sign
        real_part = real_part.reshape(quads, points, LANES)
        imag_part = imag_part.reshape(quads, points, LANES)
        new_real = real_part * cos - imag_part * sin
        new_imag = imag_part * cos + real_part * sin
        return new_real.reshape(tall, LANES), new_imag.reshape(tall, LANES)

    def dot(a, b):
        return jnp.dot(a, b, preferred_element_type=jnp.float32)

    def from_left(matrix, values):
        high, low = split(values)
        return dot(matrix, jnp.concatenate([high, high, low], axis=0))

    def from_right(values, matrix):
        high, low = split(values)
        return dot(jnp.concatenate([high, high, low], axis=1), matrix)

    def window_body(w, carry):
        slot = info[windows + w]

        def band_body(b, carry):
            orbital = w * bands + b
            for part in range(2):
                for h in range(2):
                    other[part, h] = load(orbital, part, h)
            inputs = ([], [])
            for r in range(rows):
                fields = []
                for h in range(2):
                    real_part = own[r, 0, h] * other[0, h] + own[r, 1, h] * other[1, h]
                    imag_part = own[r, 1, h] * other[0, h] - own[r, 0, h] * other[1, h]
                    fields.append(jnp.concatenate([real_part, imag_part], axis=0))
                inputs[0].append(fields[0] + fields[1])
                inputs[1].append(fields[0] - fields[1])
            turned = []
            for p in range(2):
                spectrum = from_left(left[p], jnp.concatenate(inputs[p], axis=1))
                for r in range(rows):
                    cut = spectrum[:, r * LANES:(r + 1) * LANES]
                    turned.append(jnp.concatenate(rotate(cut[:tall], cut[tall:], p, 1.0), axis=1))
            back = ([], [])
            for p in range(2):
                chosen = kernel[slot, p * tall:(p + 1) * tall, :]
                chosen = jnp.concatenate([chosen, chosen], axis=1)
                for r in range(rows):
                    full = from_right(turned[p * rows + r], right[...]) * chosen
                    full = from_right(full, right_back[...])
                    pair = rotate(full[:, :LANES], full[:, LANES:], p, -1.0)
                    back[p].append(jnp.concatenate(pair, axis=0))
            halves = [from_left(left_back[p], jnp.concatenate(back[p], axis=1)) for p in range(2)]
            for h in range(2):
                potential = halves[0] + halves[1] if h == 0 else halves[0] - halves[1]
                for r in range(rows):
                    real_part = potential[:tall, r * LANES:(r + 1) * LANES]
                    imag_part = potential[tall:, r * LANES:(r + 1) * LANES]
                    total[r, 0, h] += other[0, h] * real_part - other[1, h] * imag_part
                    total[r, 1, h] += other[0, h] * imag_part + other[1, h] * real_part
            return carry

        return lax.fori_loop(0, info[w], band_body, carry)

    lax.fori_loop(0, windows, window_body, 0)
    for r in range(rows):
        for part in range(2):
            for h in range(2):
                out[:, r, part, h * piece:(h + 1) * piece, :] = total[r, part, h].reshape(members, piece, LANES)

    def project(a, carry):
        for part in range(2):
            for h in range(2):
                other[part, h] = load(first_band + a, part, h)
        for r in range(rows):
            real_sum = jnp.zeros((tall, LANES), jnp.float32)
            imag_sum = jnp.zeros((tall, LANES), jnp.float32)
            for h in range(2):
                real_sum += other[0, h] * total[r, 0, h] + other[1, h] * total[r, 1, h]
                imag_sum += other[0, h] * total[r, 1, h] - other[1, h] * total[r, 0, h]
            projections[r, a] = jnp.concatenate(
                [jnp.sum(real_sum, axis=0, keepdims=True), jnp.sum(imag_sum, axis=0, keepdims=True)], axis=0)
        return carry

    lax.fori_loop(0, bands, project, 0)


def on_device(orbitals, band_counts, pair_slot, kernel):
    local, bands, _, planes, columns = orbitals.shape
    slots, points = kernel.shape[0], kernel.shape[1]
    members = lax.axis_size("ga")
    groups = lax.axis_size("ka")
    kpoints = local * groups
    group, member = lax.axis_index("ka"), lax.axis_index("ga")
    volume = float(points ** 3)
    wide = LANES // points
    quads = points // (2 * wide)
    tiles = columns // LANES
    rows = max(1, local * bands // members)
    share = max(1, members // (local * bands))
    windows = STEPS * local
    tables = build_tables(points, members)

    pieces = orbitals.reshape(local * bands, 2, planes, tiles, LANES).transpose(0, 1, 3, 2, 4)
    pieces = pieces.reshape(local * bands, 2, tiles * planes, LANES)
    blocks = [pieces]
    pairs = [(source, (source + 1) % groups) for source in range(groups)]
    for _ in range(STEPS - 1):
        blocks.append(lax.ppermute(blocks[-1], "ka", pairs))
    gathered = lax.all_gather(jnp.concatenate(blocks, axis=0), "ga", axis=0)

    whole = lax.all_gather(kernel, "ga", axis=2, tiled=True) * (-1.0 / (kpoints * volume))
    whole = whole.reshape(slots, points, wide, quads, 2, points).transpose(0, 4, 3, 1, 2, 5)
    whole = whole.reshape(slots, 2 * quads * points, LANES)

    first_row = member // share * rows
    own_kpoint = first_row // bands
    anchors = (group - jnp.arange(STEPS, dtype=jnp.int32)) % groups
    window = (anchors[:, None] * local + jnp.arange(local, dtype=jnp.int32)[None, :]).reshape(-1)
    slot_row = lax.dynamic_index_in_dim(pair_slot, group * local + own_kpoint, 0, keepdims=False)
    mine = jnp.arange(windows, dtype=jnp.int32) % share == member % share
    info = jnp.concatenate([jnp.where(mine, band_counts[window], 0), slot_row[window],
                            jnp.stack([first_row, own_kpoint * bands]).astype(jnp.int32)])

    tall = quads * points
    field = (rows, 2, 2, tall, LANES)
    smem = pl.BlockSpec(memory_space=pltpu.SMEM)
    vmem = pl.BlockSpec(memory_space=pltpu.VMEM)

    def body(*refs):
        pair_kernel(rows, bands, windows, points, *refs)

    spread, projections = pl.pallas_call(
        body,
        out_shape=(jax.ShapeDtypeStruct((members, rows, 2, tiles * planes, LANES), jnp.float32),
                   jax.ShapeDtypeStruct((rows, bands, 2, LANES), jnp.float32)),
        in_specs=[smem] + [vmem] * 7,
        out_specs=(vmem, vmem),
        scratch_shapes=[pltpu.VMEM(field, jnp.float32), pltpu.VMEM(field[1:], jnp.float32),
                        pltpu.VMEM(field, jnp.float32)],
        compiler_params=pltpu.CompilerParams(vmem_limit_bytes=48 * 2 ** 20),
        name="pairs",
    )(info, gathered, whole, *[jnp.asarray(table) for table in tables])

    copies = jnp.broadcast_to(projections.transpose(0, 2, 1, 3)[None], (members, rows, 2, bands, LANES))
    arrived = lax.all_to_all(jnp.concatenate([spread, copies], axis=3), "ga", split_axis=0, concat_axis=0, tiled=True)
    arrived = arrived.reshape(members * rows, 2, tiles * planes + bands, LANES)
    vectors = arrived[:, :, :tiles * planes]
    projections = arrived[:, :, tiles * planes:].reshape(local * bands, share, 2, bands, LANES).transpose(0, 1, 3, 2, 4)
    if share > 1:
        vectors = jnp.sum(vectors.reshape(local * bands, share, *vectors.shape[1:]), axis=1)
    vectors = vectors.reshape(local, bands, 2, tiles, planes, LANES).transpose(0, 1, 2, 4, 3, 5)
    vectors = vectors.reshape(local, bands, 2, planes, columns)
    sums = jnp.sum(jnp.sum(projections, axis=-1) / volume, axis=1)
    matrix = sums.reshape(local, bands, bands, 2).transpose(0, 3, 2, 1)
    own_counts = lax.dynamic_slice_in_dim(band_counts, group * local, local)
    occupied = (jnp.arange(bands)[None, :] < own_counts[:, None]).astype(jnp.float32)
    part = jnp.sum(occupied * jnp.diagonal(matrix[:, 0], axis1=1, axis2=2)) / (2.0 * kpoints)
    place = jnp.arange(groups, dtype=jnp.int32)
    terms = jnp.where(place == group, part, 0.0)
    for step in range(1, groups):
        ring = [(source, (source + step) % groups) for source in range(groups)]
        arrived = lax.ppermute(part.reshape(1), "ka", ring)
        terms = jnp.where(place == (group - step) % groups, arrived, terms)
    energy = jnp.sum(terms)
    return (vectors, matrix, energy)


def solution(mesh):
    in_specs = (P("ka", None, None, "ga", None), P(), P(), P(None, None, "ga"))
    out_specs = (P("ka", None, None, "ga", None), P("ka", None, None, None), P())
    return jax.shard_map(
        on_device, mesh=mesh, in_specs=in_specs, out_specs=out_specs, check_vma=False
    )
```
